32 devices in a mesh: lang: 2 (over y), clu: 16 (over z, x, core).
Axes of the slice: x: 2, y: 2, z: 4, core: 2. Of those that a mesh axis runs over, the one named last changes fastest.
Arguments:
- embeddings: bfloat16 [8192, 1024], P(('lang', 'clu')), parts along dimension 0, may hold values from -6 to 6
- assignment: int32 [8192, 1], P(('lang', 'clu')), parts along dimension 0, may hold values from 0 to 31; in each aligned block of 256 rows (0 to 255, 256 to 511, ...) at most 16 rows name the same one
Outputs:
- best_similarity: float32 [8192], P(('lang', 'clu')), parts along dimension 0
The draws below stay inside these ranges and needn't reach their ends.
There are 2 independent parts, one for each index of `lang`. The reference program is written for one: setup_inputs(seed, part) draws one part's arguments, and reference() takes and returns one part's arrays. A program takes and returns all parts, laid end to end along the dimension named above; each array names one. Nothing has to cross between parts.
Inputs may be any that keep to these rules, and one draw needn't show every extreme that they name: `assignment`: in each aligned block of 256 rows (the rows of one device) no cluster is named by more than 16 rows; every cluster is named by some row.
All inputs are finite; a program needn't handle non-finite values.
Results may differ from the reference program's by a relative error of at most 0.0016.
Values may be sent and summed in bfloat16 or wider, within the bound.
No kernel may reach another device: no remote copies, remote signals or barrier semaphores. Data moves between devices by JAX's collectives and lax.ppermute only.
A program may use at most 64 MiB of HBM per device.

```python
import math
import jax
import jax.numpy as jnp
import numpy as np
from jax import lax

D = 1024
ROWS_DEV = 256
CLUSTERS = 32
MOST = 16
ROWS = 4096
N_CLU = 16


def shard_levels(rng, extent, shards, least, top_value):
    level = 1.0
    for dim, blocks in shards:
        draws = jax.random.uniform(jax.random.fold_in(jax.random.fold_in(rng, 6), dim), (blocks,), jnp.float32, least / len(shards), top_value / len(shards))
        level = level * jnp.repeat(jnp.exp(draws), extent[dim] // blocks).reshape((-1,) + (1,) * (len(extent) - 1 - dim))
    return level


def deal_out(rng, own, number, rows, amount, top, most, skew):
    ranking = jax.random.permutation(rng, amount)
    crowded, common = portions_of(amount, rows * top, most, skew, True), portions_of(amount, rows * top, most, skew, False)
    places = jnp.arange(amount)

    def named(sizes, turn):
        used = int((sizes > 0).sum())
        fixed = max(1, used // 4)
        moved = fixed + (places - fixed + turn * (used - fixed)) % max(1, amount - fixed)
        return jnp.zeros((amount,), jnp.int32).at[ranking[jnp.where(places < fixed, places, moved)]].set(jnp.asarray(sizes, jnp.int32))

    sizes = jnp.where(number % 4 == 0, named(crowded, number // 4), named(common, number - number // 4 - 1))
    mixed = jax.random.permutation(jax.random.fold_in(own, 3), amount)
    donor, taker = mixed[0:amount // 2 * 2:2], mixed[1:amount // 2 * 2:2]
    margin = jnp.minimum(sizes[donor] - 1, most - sizes[taker]) // 2
    margin = jnp.where((donor == ranking[0]) | (taker == ranking[0]) | (sizes[taker] == 0), 0, jnp.maximum(margin, 0))
    moved = jax.random.randint(jax.random.fold_in(own, 4), (amount // 2,), 0, 1 << 20) % (margin + 1)
    sizes = sizes.at[donor].add(-moved).at[taker].add(moved)
    items = jnp.searchsorted(jnp.cumsum(sizes), jnp.arange(rows * top), side="right").astype(jnp.int32)
    table = items.reshape(top, rows).T
    table = table[jax.random.permutation(jax.random.fold_in(own, 1), rows)]
    turn = jax.random.randint(jax.random.fold_in(own, 2), (rows, 1), 0, top)
    return jnp.take_along_axis(table, (jnp.arange(top)[None, :] + turn) % top, axis=1)


def portions_of(number_of, total, reach, slope, full):
    weights = [(1 << 20) // math.isqrt(standing ** slope) + 1 for standing in range(1, number_of + 1)]
    largest = reach if full else min(reach, max(-(-total // number_of), total * weights[0] // sum(weights)))
    least = 1 if total - largest >= number_of - 1 else 0
    holding, surplus = [largest] + [least] * (number_of - 1), total - largest - least * (number_of - 1)
    while surplus > 0:
        movable = [i for i in range(1, number_of) if holding[i] < largest] or [i for i in range(1, number_of) if holding[i] < reach]
        mass, budget = sum([weights[i] for i in movable]), surplus
        for i in movable:
            extra = min(reach - holding[i], max(1, budget * weights[i] // mass), surplus)
            holding[i] = holding[i] + extra
            surplus = surplus - extra
    return np.array(holding)


def bell_draw(own_key, dims, deviation, most, pieces=(), kind=jnp.bfloat16):
    gain = shard_levels(own_key, dims, pieces, -0.22, 0.18) if pieces else 1.0
    drawn = jax.random.normal(own_key, dims, jnp.float32) * deviation * gain
    return jnp.minimum(jnp.maximum(drawn, -most), most).astype(kind)


def setup_inputs(seed: int = 0, part: int = 0) -> dict:
    splits = jax.random.split(jax.random.key(seed), 3)
    part_splits = jax.random.split(jax.random.fold_in(splits[2], part), 3)
    embeddings = bell_draw(part_splits[0], (ROWS, D), 1.0, 6.0, ((0, 16),))
    assignment_keys = jax.random.split(jax.random.fold_in(part_splits[1], 1), ROWS // ROWS_DEV)
    assignment_turns = jax.random.permutation(jax.random.fold_in(part_splits[1], 3), ROWS // ROWS_DEV)
    assignment = jax.vmap(lambda own, number: deal_out(jax.random.fold_in(part_splits[1], 2), own, number, ROWS_DEV, CLUSTERS, 1, MOST, 2))(assignment_keys, assignment_turns).reshape((ROWS, 1))
    return {"embeddings": embeddings, "assignment": assignment}


EPS = 1e-06

def normalize(embeddings):
    values = embeddings.astype(jnp.float32)
    scale = lax.rsqrt(lax.optimization_barrier(jnp.sum(values * values, axis=-1, keepdims=True)) + EPS)
    return (values * scale).astype(jnp.bfloat16)

def reference(embeddings, assignment):
    unit = normalize(embeddings)
    cluster = assignment[:, 0].astype(jnp.int32)
    total = cluster.shape[0]
    order = jnp.argsort(cluster, stable=True).astype(jnp.int32)
    ranked = cluster[order]
    labels = jnp.arange(CLUSTERS, dtype=jnp.int32)
    starts = jnp.searchsorted(ranked, labels, side='left').astype(jnp.int32)
    ends = jnp.searchsorted(ranked, labels, side='right').astype(jnp.int32)
    sorted_unit = unit[order]
    width = N_CLU * MOST
    offsets = jnp.arange(width, dtype=jnp.int32)
    distinct = offsets[:, None] != offsets[None, :]

    def score(label):
        index = jnp.clip(starts[label] + offsets, 0, total - 1).astype(jnp.int32)
        live = offsets < ends[label] - starts[label]
        rows = sorted_unit[index]
        gram = jnp.dot(rows, rows.T, preferred_element_type=jnp.float32)
        keep = distinct & live[None, :]
        best = lax.optimization_barrier(jnp.max(jnp.where(keep, gram, jnp.float32(-2.0)), axis=1))
        return jnp.maximum(best, jnp.float32(-1.0))
    table = lax.map(score, labels)
    position = jnp.arange(total, dtype=jnp.int32)
    inside = (position - starts[ranked]).astype(jnp.int32)
    sorted_best = table[ranked, inside]
    return jnp.zeros((total,), jnp.float32).at[order].set(sorted_best)
```

```python
import functools

import jax
import jax.numpy as jnp
from jax import lax
from jax.experimental import pallas as pl
from jax.experimental.pallas import tpu as pltpu
from jax.sharding import PartitionSpec as P

CLU_DEV = 2
EPS = 1e-06
PAD = 2.0
LANES = 128


def pack_kernel(most, rows_ref, cluster_ref, out_ref, slot_ref):
    count = rows_ref.shape[0]
    slots = out_ref.shape[0]
    labels = slots // most
    cluster = cluster_ref[...]
    member = lax.broadcasted_iota(jnp.int32, (labels, count), 0) == cluster
    onehot = member.astype(jnp.bfloat16)
    before = (
        lax.broadcasted_iota(jnp.int32, (count, count), 0)
        < lax.broadcasted_iota(jnp.int32, (count, count), 1)
    ).astype(jnp.bfloat16)
    prior = jnp.dot(onehot, before, preferred_element_type=jnp.float32)
    rank = jnp.sum(jnp.where(member, prior, 0.0), axis=0, keepdims=True)
    slot = cluster * most + rank.astype(jnp.int32)
    slot_ref[...] = slot
    place = (lax.broadcasted_iota(jnp.int32, (slots, count), 0) == slot).astype(jnp.bfloat16)
    values = rows_ref[...].astype(jnp.float32)
    scale = lax.rsqrt(jnp.sum(values * values, axis=-1, keepdims=True) + EPS)
    unit = (values * scale).astype(jnp.bfloat16)
    packed = jnp.dot(place, unit, preferred_element_type=jnp.float32)
    live = jnp.sum(place.astype(jnp.float32), axis=1, keepdims=True) > 0
    first = lax.broadcasted_iota(jnp.int32, packed.shape, 1) == 0
    out_ref[...] = jnp.where(first & ~live, PAD, packed).astype(jnp.bfloat16)


def score_kernel(most, rows_ref, out_ref):
    slots = rows_ref.shape[0]
    groups = out_ref.shape[0]
    rows = rows_ref[...]
    gram = lax.dot_general(
        rows, rows, (((1,), (1,)), ((), ())), preferred_element_type=jnp.float32
    )
    live = rows[:, :1].astype(jnp.float32) < 1.5
    i = lax.broadcasted_iota(jnp.int32, (slots, slots), 0)
    j = lax.broadcasted_iota(jnp.int32, (slots, slots), 1)
    keep = live & (i != j) & (((i // most) ^ (j // most)) % CLU_DEV == 0)
    best = jnp.max(jnp.where(keep, gram, -1.0), axis=0, keepdims=True)
    share = LANES * groups // slots
    for p in range(groups):
        out_ref[p] = best[:, p // share * LANES : (p // share + 1) * LANES]


def pick_kernel(best_ref, slot_ref, out_ref):
    groups = best_ref.shape[0]
    count = slot_ref.shape[1]
    width = 2 * count // groups
    slot = slot_ref[...]
    lane = lax.axis_index("clu") % (LANES // width) * width + slot % width
    inner = (lax.broadcasted_iota(jnp.int32, (LANES, count), 0) == lane).astype(jnp.float32)
    table = jnp.dot(
        best_ref[:, 0, :], inner, precision=lax.Precision.HIGHEST,
        preferred_element_type=jnp.float32,
    )
    outer = lax.broadcasted_iota(jnp.int32, (groups, count), 0) == slot // width
    out_ref[...] = jnp.sum(jnp.where(outer, table, 0.0), axis=0, keepdims=True)


def shards(embeddings, assignment):
    groups = lax.axis_size("clu")
    count, width = embeddings.shape
    most = 2 * count // (CLU_DEV * groups)
    slots = CLU_DEV * groups * most
    vmem = pl.BlockSpec(memory_space=pltpu.VMEM)
    packed, slot = pl.pallas_call(
        functools.partial(pack_kernel, most),
        out_shape=(
            jax.ShapeDtypeStruct((slots, width), jnp.bfloat16),
            jax.ShapeDtypeStruct((1, count), jnp.int32),
        ),
        in_specs=[vmem, vmem],
        out_specs=(vmem, vmem),
        name="pack",
    )(embeddings, assignment.reshape(1, count))
    packed = packed.reshape(groups, CLU_DEV * most, width)
    arrived = lax.all_to_all(packed, "clu", split_axis=0, concat_axis=0, tiled=True)
    best = pl.pallas_call(
        functools.partial(score_kernel, most),
        out_shape=jax.ShapeDtypeStruct((groups, 1, LANES), jnp.float32),
        in_specs=[vmem],
        out_specs=vmem,
        name="score",
    )(arrived.reshape(slots, width))
    returned = lax.all_to_all(best, "clu", split_axis=0, concat_axis=0, tiled=True)
    out = pl.pallas_call(
        pick_kernel,
        out_shape=jax.ShapeDtypeStruct((1, count), jnp.float32),
        in_specs=[vmem, vmem],
        out_specs=vmem,
        name="pick",
    )(returned, slot)
    return out.reshape(count)


def solution(mesh):
    in_specs = (P(("lang", "clu"), None), P(("lang", "clu"), None))
    out_specs = P(("lang", "clu"))
    return jax.shard_map(shards, mesh=mesh, in_specs=in_specs, out_specs=out_specs, check_vma=False)
```

```python
import functools

import jax
import jax.numpy as jnp
from jax import lax
from jax.experimental import pallas as pl
from jax.experimental.pallas import tpu as pltpu
from jax.sharding import PartitionSpec as P


CLU_DEV = 2
EPS = 1e-06
PAD = 2.0
LANES = 128
GRANT = 8 * 1024 * 1024
VMEM = pl.BlockSpec(memory_space=pltpu.VMEM)
HBM = pl.BlockSpec(memory_space=pltpu.HBM)


def call(kernel, out_shape, args, in_specs=None, scratch=(), flops=1 << 24, grant=GRANT):
    return pl.pallas_call(
        kernel,
        out_shape=out_shape,
        in_specs=in_specs or [VMEM] * len(args),
        out_specs=jax.tree.map(lambda _: VMEM, out_shape),
        scratch_shapes=scratch,
        compiler_params=pltpu.CompilerParams(vmem_limit_bytes=grant),
        cost_estimate=pl.CostEstimate(flops=flops, bytes_accessed=1 << 20, transcendentals=0),
    )(*args)


def block_order(k):
    return k ^ jnp.where(k >= 2, 1, 0)


def rank_of(cluster, labels):
    count = cluster.shape[1]
    member = lax.broadcasted_iota(jnp.int32, (labels, count), 0) == cluster
    before = (
        lax.broadcasted_iota(jnp.int32, (count, count), 0)
        < lax.broadcasted_iota(jnp.int32, (count, count), 1)
    ).astype(jnp.bfloat16)
    prior = jnp.dot(member.astype(jnp.bfloat16), before, preferred_element_type=jnp.float32)
    return jnp.sum(jnp.where(member, prior, 0.0), axis=0, keepdims=True).astype(jnp.int32)


def pack_kernel(sizes, most, labels, relative, rows_hbm, cluster_hbm, *refs):
    *out_refs, rank_ref, cluster_ref, rows_ref, cluster_vmem, sems = refs
    load_cluster = pltpu.make_async_copy(cluster_hbm, cluster_vmem, sems.at[0])
    load_rows = pltpu.make_async_copy(rows_hbm, rows_ref, sems.at[1])
    load_cluster.start()
    load_rows.start()
    load_cluster.wait()
    cluster = cluster_vmem[...]
    rank = rank_of(cluster, labels)
    rank_ref[...] = rank
    cluster_ref[...] = cluster
    owner = cluster // CLU_DEV
    if relative:
        owner = block_order(owner ^ lax.axis_index("clu"))
    position = (owner * CLU_DEV + cluster % CLU_DEV) * most + rank
    slots = sum(sizes)
    count = rows_ref.shape[0]
    place = lax.broadcasted_iota(jnp.int32, (slots, count), 0) == position
    live = jnp.sum(place.astype(jnp.float32), axis=1, keepdims=True) > 0
    load_rows.wait()
    values = rows_ref[...].astype(jnp.float32)
    scale = lax.rsqrt(jnp.sum(values * values, axis=-1, keepdims=True) + EPS)
    unit = (values * scale).astype(jnp.bfloat16)
    packed = jnp.dot(place.astype(jnp.bfloat16), unit, preferred_element_type=jnp.float32)
    first = lax.broadcasted_iota(jnp.int32, (slots, LANES), 1) == 0
    head = jnp.where(first & ~live, PAD, packed[:, :LANES]).astype(jnp.bfloat16)
    rest = packed[:, LANES:].astype(jnp.bfloat16)
    start = 0
    for size, out_ref in zip(sizes, out_refs):
        out_ref[:, :LANES] = head[start:start + size]
        out_ref[:, LANES:] = rest[start:start + size]
        start += size


def best_of(rows, keep=None):
    slots = rows.shape[0]
    gram = lax.dot_general(
        rows, rows, (((1,), (1,)), ((), ())), preferred_element_type=jnp.float32
    )
    live = rows[:, :1].astype(jnp.float32) < 1.5
    i = lax.broadcasted_iota(jnp.int32, (slots, slots), 0)
    j = lax.broadcasted_iota(jnp.int32, (slots, slots), 1)
    mask = live & (i != j)
    if keep is not None:
        mask &= keep(i, j)
    return jnp.max(jnp.where(mask, gram, -1.0), axis=0, keepdims=True)


def score_blocks_kernel(most, where, *refs):
    *row_refs, out_ref = refs
    me = lax.axis_index("clu")
    for local in range(CLU_DEV):
        rows = jnp.concatenate(
            [row_refs[n][start + local * most:start + (local + 1) * most] for n, start in where],
            axis=0,
        )
        best = best_of(rows)
        for k in range(len(where)):
            lane = k * most // LANES * LANES
            out_ref[me ^ k, pl.ds(local, 1), :] = best[:, lane:lane + LANES]


def score_all_kernel(most, rows_ref, out_ref):
    groups = out_ref.shape[0]
    best = best_of(rows_ref[...], lambda i, j: ((i // most) ^ (j // most)) % CLU_DEV == 0)
    share = LANES // (CLU_DEV * most)
    for p in range(groups):
        out_ref[p] = best[:, p // share * LANES:(p // share + 1) * LANES]


def pick_kernel(most, relative, best_ref, rank_ref, cluster_ref, out_ref):
    groups, lines = best_ref.shape[:2]
    count = rank_ref.shape[1]
    me = lax.axis_index("clu")
    cluster = cluster_ref[...]
    owner = cluster // CLU_DEV
    local = cluster % CLU_DEV
    if relative:
        lane = (owner ^ me) * most + rank_ref[...]
    else:
        lane = (me * CLU_DEV + local) * most + rank_ref[...]
    inner = (lax.broadcasted_iota(jnp.int32, (LANES, count), 0) == lane % LANES).astype(jnp.float32)
    total = jnp.zeros((1, count), jnp.float32)
    for line in range(lines):
        table = jnp.dot(
            best_ref[:, line, :], inner, precision=lax.Precision.HIGHEST,
            preferred_element_type=jnp.float32,
        )
        outer = lax.broadcasted_iota(jnp.int32, (groups, count), 0) == owner
        if lines > 1:
            outer &= local == line
        total += jnp.sum(jnp.where(outer, table, 0.0), axis=0, keepdims=True)
    out_ref[...] = total


def pack(embeddings, assignment, sizes, most, labels, relative):
    count, width = embeddings.shape
    line = jax.ShapeDtypeStruct((1, count), jnp.int32)
    out = tuple(jax.ShapeDtypeStruct((size, width), jnp.bfloat16) for size in sizes)
    *packed, rank, cluster = call(
        functools.partial(pack_kernel, sizes, most, labels, relative),
        (*out, line, line),
        (
            pltpu.with_memory_space_constraint(embeddings, pltpu.HBM),
            pltpu.with_memory_space_constraint(assignment.reshape(1, count), pltpu.HBM),
        ),
        in_specs=[HBM, HBM],
        scratch=[
            pltpu.VMEM((count, width), jnp.bfloat16),
            pltpu.VMEM((1, count), jnp.int32),
            pltpu.SemaphoreType.DMA((2,)),
        ],
    )
    return packed, rank, cluster


def swap(array, k):
    groups = lax.axis_size("clu")
    return lax.ppermute(array, "clu", [(i, i ^ k) for i in range(groups)])


def exchange_blocks(embeddings, assignment, most, labels):
    groups = lax.axis_size("clu")
    block = CLU_DEV * most
    chips = groups // 2
    last = chips // 2
    sizes = [block, block]
    for m in range(1, chips):
        sizes += [block, block] if m == last else [2 * block]
    packed, rank, cluster = pack(embeddings, assignment, tuple(sizes), most, labels, True)
    own, partner, *others = packed
    sent = {}
    for m in range(1, chips):
        sent[m] = [others.pop(0) for _ in range(2 if m == last else 1)]
    arrived = {}
    for m in range(1, chips):
        arrived[m] = []
        for n, array in enumerate(sent[m]):
            arrived[m].append(swap(array, 2 * m + 1 - n))
    args = [own, swap(partner, 1)]
    where = [(0, 0), (1, 0)]
    for m in range(1, chips):
        if m == last:
            far, near = arrived[m]
            args += [near, far]
            where += [(len(args) - 2, 0), (len(args) - 1, 0)]
        else:
            both = arrived[m][0]
            args += [swap(both[block:], 1), both]
            where += [(len(args) - 2, 0), (len(args) - 1, 0)]
    best = call(
        functools.partial(score_blocks_kernel, most, tuple(where)),
        jax.ShapeDtypeStruct((groups, CLU_DEV, LANES), jnp.float32), args,
    )
    return best, rank, cluster


def exchange_all(embeddings, assignment, most, labels):
    groups = lax.axis_size("clu")
    width = embeddings.shape[1]
    slots = labels * most
    (packed,), rank, cluster = pack(embeddings, assignment, (slots,), most, labels, False)
    arrived = lax.all_to_all(
        packed.reshape(groups, slots // groups, width), "clu",
        split_axis=0, concat_axis=0, tiled=True,
    )
    best = call(
        functools.partial(score_all_kernel, most),
        jax.ShapeDtypeStruct((groups, 1, LANES), jnp.float32), (arrived.reshape(slots, width),),
    )
    return best, rank, cluster


def uses_blocks(groups, most):
    return most % 16 == 0 and groups >= 4 and groups & (groups - 1) == 0


def shards(embeddings, assignment):
    groups = lax.axis_size("clu")
    count = embeddings.shape[0]
    most = 2 * count // (CLU_DEV * groups)
    labels = CLU_DEV * groups
    relative = uses_blocks(groups, most)
    exchange = exchange_blocks if relative else exchange_all
    best, rank, cluster = exchange(embeddings, assignment, most, labels)
    returned = lax.all_to_all(best, "clu", split_axis=0, concat_axis=0, tiled=True)
    out = call(
        functools.partial(pick_kernel, most, relative),
        jax.ShapeDtypeStruct((1, count), jnp.float32), (returned, rank, cluster),
    )
    return out.reshape(count)


def solution(mesh):
    in_specs = (P(("lang", "clu"), None), P(("lang", "clu"), None))
    out_specs = P(("lang", "clu"))

    return jax.shard_map(shards, mesh=mesh, in_specs=in_specs, out_specs=out_specs, check_vma=False)
```

```python
import functools

import jax
import jax.numpy as jnp
from jax import lax
from jax.experimental import pallas as pl
from jax.experimental.pallas import tpu as pltpu
from jax.sharding import PartitionSpec as P


CLU_DEV = 2
EPS = 1e-06
PAD = 2.0
LANES = 128
GRANT = 8 * 1024 * 1024
VMEM = pl.BlockSpec(memory_space=pltpu.VMEM)
HBM = pl.BlockSpec(memory_space=pltpu.HBM)


def call(kernel, out_shape, args, in_specs=None, scratch=(), flops=1 << 24, grant=GRANT):
    return pl.pallas_call(
        kernel,
        out_shape=out_shape,
        in_specs=in_specs or [VMEM] * len(args),
        out_specs=jax.tree.map(lambda _: VMEM, out_shape),
        scratch_shapes=scratch,
        compiler_params=pltpu.CompilerParams(vmem_limit_bytes=grant),
        cost_estimate=pl.CostEstimate(flops=flops, bytes_accessed=1 << 20, transcendentals=0),
    )(*args)


def block_order(k):
    return k ^ jnp.where(k >= 2, 1, 0)


def rank_of(cluster, labels):
    count = cluster.shape[1]
    member = lax.broadcasted_iota(jnp.int32, (labels, count), 0) == cluster
    before = (
        lax.broadcasted_iota(jnp.int32, (count, count), 0)
        < lax.broadcasted_iota(jnp.int32, (count, count), 1)
    ).astype(jnp.bfloat16)
    prior = jnp.dot(member.astype(jnp.bfloat16), before, preferred_element_type=jnp.float32)
    return jnp.sum(jnp.where(member, prior, 0.0), axis=0, keepdims=True).astype(jnp.int32)


def pack_kernel(sizes, most, labels, relative, rows_hbm, cluster_hbm, *refs):
    *out_refs, rank_ref, cluster_ref, rows_ref, cluster_vmem, sems = refs
    load_cluster = pltpu.make_async_copy(cluster_hbm, cluster_vmem, sems.at[0])
    load_rows = pltpu.make_async_copy(rows_hbm, rows_ref, sems.at[1])
    load_cluster.start()
    load_rows.start()
    load_cluster.wait()
    cluster = cluster_vmem[...]
    rank = rank_of(cluster, labels)
    rank_ref[...] = rank
    cluster_ref[...] = cluster
    owner = cluster // CLU_DEV
    if relative:
        owner = block_order(owner ^ lax.axis_index("clu"))
    position = (owner * CLU_DEV + cluster % CLU_DEV) * most + rank
    slots = sum(sizes)
    count = rows_ref.shape[0]
    place = lax.broadcasted_iota(jnp.int32, (slots, count), 0) == position
    live = jnp.sum(place.astype(jnp.float32), axis=1, keepdims=True) > 0
    load_rows.wait()
    values = rows_ref[...].astype(jnp.float32)
    scale = lax.rsqrt(jnp.sum(values * values, axis=-1, keepdims=True) + EPS)
    unit = (values * scale).astype(jnp.bfloat16)
    packed = jnp.dot(place.astype(jnp.bfloat16), unit, preferred_element_type=jnp.float32)
    first = lax.broadcasted_iota(jnp.int32, (slots, LANES), 1) == 0
    head = jnp.where(first & ~live, PAD, packed[:, :LANES]).astype(jnp.bfloat16)
    rest = packed[:, LANES:].astype(jnp.bfloat16)
    start = 0
    for size, out_ref in zip(sizes, out_refs):
        out_ref[:, :LANES] = head[start:start + size]
        out_ref[:, LANES:] = rest[start:start + size]
        start += size


def best_of(rows, keep=None):
    slots = rows.shape[0]
    gram = lax.dot_general(
        rows, rows, (((1,), (1,)), ((), ())), preferred_element_type=jnp.float32
    )
    live = rows[:, :1].astype(jnp.float32) < 1.5
    i = lax.broadcasted_iota(jnp.int32, (slots, slots), 0)
    j = lax.broadcasted_iota(jnp.int32, (slots, slots), 1)
    mask = live & (i != j)
    if keep is not None:
        mask &= keep(i, j)
    return jnp.max(jnp.where(mask, gram, -1.0), axis=0, keepdims=True)


def score_blocks_kernel(most, where, *refs):
    *row_refs, out_ref = refs
    me = lax.axis_index("clu")
    best = []
    for local in range(CLU_DEV):
        rows = jnp.concatenate(
            [row_refs[n][start + local * most:start + (local + 1) * most] for n, start in where],
            axis=0,
        )
        best.append(best_of(rows))
    share = LANES // most
    group = lax.broadcasted_iota(jnp.int32, (1, LANES), 1) // most
    for base in range(0, len(where), share):
        lane = base * most
        low = best[0][:, lane:lane + LANES]
        high = pltpu.roll(best[1][:, lane:lane + LANES], most, 1)
        for parity in range(2):
            line = jnp.where(group % 2 == parity, low, high)
            for k in range(base + parity, base + share, 2):
                out_ref[me ^ k] = line


def score_all_kernel(most, rows_ref, out_ref):
    groups = out_ref.shape[0]
    best = best_of(rows_ref[...], lambda i, j: ((i // most) ^ (j // most)) % CLU_DEV == 0)
    share = LANES // (CLU_DEV * most)
    for p in range(groups):
        out_ref[p] = best[:, p // share * LANES:(p // share + 1) * LANES]


def pick_kernel(most, relative, best_ref, rank_ref, cluster_ref, out_ref):
    groups = best_ref.shape[0]
    count = rank_ref.shape[1]
    me = lax.axis_index("clu")
    cluster = cluster_ref[...]
    owner = cluster // CLU_DEV
    local = cluster % CLU_DEV
    if relative:
        lane = ((owner ^ me) + local) * most + rank_ref[...]
    else:
        lane = (me * CLU_DEV + local) * most + rank_ref[...]
    lane = lane % LANES
    best = best_ref[:, 0, :]
    row = lax.broadcasted_iota(jnp.int32, (groups, LANES), 0)
    for start in range(0, count, LANES):
        index = jnp.broadcast_to(lane[:, start:start + LANES], (groups, LANES))
        table = jnp.take_along_axis(best, index, axis=1)
        mine = row == owner[:, start:start + LANES]
        out_ref[:, start:start + LANES] = jnp.sum(
            jnp.where(mine, table, 0.0), axis=0, keepdims=True
        )


def pack(embeddings, assignment, sizes, most, labels, relative):
    count, width = embeddings.shape
    line = jax.ShapeDtypeStruct((1, count), jnp.int32)
    out = tuple(jax.ShapeDtypeStruct((size, width), jnp.bfloat16) for size in sizes)
    *packed, rank, cluster = call(
        functools.partial(pack_kernel, sizes, most, labels, relative),
        (*out, line, line),
        (
            pltpu.with_memory_space_constraint(embeddings, pltpu.HBM),
            pltpu.with_memory_space_constraint(assignment.reshape(1, count), pltpu.HBM),
        ),
        in_specs=[HBM, HBM],
        scratch=[
            pltpu.VMEM((count, width), jnp.bfloat16),
            pltpu.VMEM((1, count), jnp.int32),
            pltpu.SemaphoreType.DMA((2,)),
        ],
    )
    return packed, rank, cluster


def swap(array, k):
    groups = lax.axis_size("clu")
    return lax.ppermute(array, "clu", [(i, i ^ k) for i in range(groups)])


def exchange_blocks(embeddings, assignment, most, labels):
    groups = lax.axis_size("clu")
    block = CLU_DEV * most
    chips = groups // 2
    last = chips // 2
    sizes = [block, block]
    for m in range(1, chips):
        sizes += [block, block] if m == last else [2 * block]
    packed, rank, cluster = pack(embeddings, assignment, tuple(sizes), most, labels, True)
    own, partner, *others = packed
    sent = {}
    for m in range(1, chips):
        sent[m] = [others.pop(0) for _ in range(2 if m == last else 1)]
    arrived = {}
    for m in range(1, chips):
        arrived[m] = []
        for n, array in enumerate(sent[m]):
            arrived[m].append(swap(array, 2 * m + 1 - n))
    args = [own, swap(partner, 1)]
    where = [(0, 0), (1, 0)]
    for m in range(1, chips):
        if m == last:
            far, near = arrived[m]
            args += [near, far]
            where += [(len(args) - 2, 0), (len(args) - 1, 0)]
        else:
            both = arrived[m][0]
            args += [swap(both[block:], 1), both]
            where += [(len(args) - 2, 0), (len(args) - 1, 0)]
    best = call(
        functools.partial(score_blocks_kernel, most, tuple(where)),
        jax.ShapeDtypeStruct((groups, 1, LANES), jnp.float32), args,
    )
    return best, rank, cluster


def exchange_all(embeddings, assignment, most, labels):
    groups = lax.axis_size("clu")
    width = embeddings.shape[1]
    slots = labels * most
    (packed,), rank, cluster = pack(embeddings, assignment, (slots,), most, labels, False)
    arrived = lax.all_to_all(
        packed.reshape(groups, slots // groups, width), "clu",
        split_axis=0, concat_axis=0, tiled=True,
    )
    best = call(
        functools.partial(score_all_kernel, most),
        jax.ShapeDtypeStruct((groups, 1, LANES), jnp.float32), (arrived.reshape(slots, width),),
    )
    return best, rank, cluster


def uses_blocks(groups, most):
    power = groups & (groups - 1) == 0
    return power and groups >= 16 and most % 16 == 0 and LANES % (2 * most) == 0


def shards(embeddings, assignment):
    groups = lax.axis_size("clu")
    count = embeddings.shape[0]
    most = 2 * count // (CLU_DEV * groups)
    labels = CLU_DEV * groups
    relative = uses_blocks(groups, most)
    exchange = exchange_blocks if relative else exchange_all
    best, rank, cluster = exchange(embeddings, assignment, most, labels)
    returned = lax.all_to_all(best, "clu", split_axis=0, concat_axis=0, tiled=True)
    out = call(
        functools.partial(pick_kernel, most, relative),
        jax.ShapeDtypeStruct((1, count), jnp.float32), (returned, rank, cluster),
    )
    return out.reshape(count)


def solution(mesh):
    in_specs = (P(("lang", "clu"), None), P(("lang", "clu"), None))
    out_specs = P(("lang", "clu"))

    return jax.shard_map(shards, mesh=mesh, in_specs=in_specs, out_specs=out_specs, check_vma=False)
```

```python
import functools

import jax
import jax.numpy as jnp
from jax import lax
from jax.experimental import pallas as pl
from jax.experimental.pallas import tpu as pltpu
from jax.sharding import PartitionSpec as P


CLU_DEV = 2
EPS = 1e-06
PAD = 2.0
RAW_PAD = 64.0
LANES = 128
GRANT = 12 * 1024 * 1024
VMEM = pl.BlockSpec(memory_space=pltpu.VMEM)
HBM = pl.BlockSpec(memory_space=pltpu.HBM)


def call(kernel, out_shape, args, in_specs=None, scratch=(), flops=1 << 24, grant=GRANT):
    return pl.pallas_call(
        kernel,
        out_shape=out_shape,
        in_specs=in_specs or [VMEM] * len(args),
        out_specs=jax.tree.map(lambda _: VMEM, out_shape),
        scratch_shapes=scratch,
        compiler_params=pltpu.CompilerParams(vmem_limit_bytes=grant),
        cost_estimate=pl.CostEstimate(flops=flops, bytes_accessed=1 << 20, transcendentals=0),
    )(*args)


def rank_of(cluster, labels):
    count = cluster.shape[1]
    member = lax.broadcasted_iota(jnp.int32, (labels, count), 0) == cluster
    before = (
        lax.broadcasted_iota(jnp.int32, (count, count), 0)
        < lax.broadcasted_iota(jnp.int32, (count, count), 1)
    ).astype(jnp.bfloat16)
    prior = jnp.dot(member.astype(jnp.bfloat16), before, preferred_element_type=jnp.float32)
    return jnp.sum(jnp.where(member, prior, 0.0), axis=0, keepdims=True).astype(jnp.int32)


def unit_rows(rows):
    values = rows.astype(jnp.float32)
    scale = lax.rsqrt(jnp.sum(values * values, axis=-1, keepdims=True) + EPS)
    return (values * scale).astype(jnp.bfloat16)


def place_rows(first, sizes, position, rows, pad, out_refs):
    slots = sum(sizes)
    count = rows.shape[0]
    place = lax.broadcasted_iota(jnp.int32, (slots, count), 0) + first == position
    live = jnp.sum(place.astype(jnp.float32), axis=1, keepdims=True) > 0
    packed = jnp.dot(place.astype(jnp.bfloat16), rows, preferred_element_type=jnp.float32)
    column = lax.broadcasted_iota(jnp.int32, (slots, LANES), 1) == 0
    head = jnp.where(column & ~live, pad, packed[:, :LANES]).astype(jnp.bfloat16)
    rest = packed[:, LANES:].astype(jnp.bfloat16)
    start = 0
    for size, out_ref in zip(sizes, out_refs):
        out_ref[:, :LANES] = head[start:start + size]
        out_ref[:, LANES:] = rest[start:start + size]
        start += size


def pack_kernel(sizes, most, labels, block_of, rows_hbm, cluster_hbm, *refs):
    *out_refs, rows_ref, position_ref, rank_ref, cluster_ref, sems = refs
    load_cluster = pltpu.make_async_copy(cluster_hbm, cluster_ref, sems.at[0])
    load_rows = pltpu.make_async_copy(rows_hbm, rows_ref, sems.at[1])
    load_cluster.start()
    load_rows.start()
    load_cluster.wait()
    cluster = cluster_ref[...]
    rank = rank_of(cluster, labels)
    rank_ref[...] = rank
    owner = block_of(cluster // CLU_DEV)
    position = (owner * CLU_DEV + cluster % CLU_DEV) * most + rank
    position_ref[...] = position
    load_rows.wait()
    place_rows(0, sizes, position, rows_ref[...], RAW_PAD, out_refs)


def pack_rest_kernel(first, sizes, rows_ref, position_ref, *out_refs):
    place_rows(first, sizes, position_ref[...], unit_rows(rows_ref[...]), PAD, out_refs)


def fits(rows, limit):
    return rows[:, :1].astype(jnp.float32) < limit


def marked_units(rows):
    live = fits(rows, RAW_PAD / 2)
    unit = unit_rows(rows)
    column = lax.broadcasted_iota(jnp.int32, (rows.shape[0], LANES), 1) == 0
    head = jnp.where(column & ~live, PAD, unit[:, :LANES].astype(jnp.float32))
    return jnp.concatenate([head.astype(jnp.bfloat16), unit[:, LANES:]], axis=1)


def best_over(left, right, offset, keep=None):
    gram = lax.dot_general(
        left, right, (((1,), (1,)), ((), ())), preferred_element_type=jnp.float32
    )
    i = lax.broadcasted_iota(jnp.int32, gram.shape, 0)
    j = lax.broadcasted_iota(jnp.int32, gram.shape, 1)
    mask = fits(left, PAD * 0.75) & (i + offset != j)
    if keep is not None:
        mask &= keep(i, j)
    return jnp.max(jnp.where(mask, gram, -1.0), axis=0, keepdims=True)


def units_kernel(*refs):
    half = len(refs) // 2
    for row_ref, out_ref in zip(refs[:half], refs[half:]):
        out_ref[...] = marked_units(row_ref[:out_ref.shape[0]])


def score_blocks_kernel(most, where, *refs):
    *row_refs, out_ref = refs
    me = lax.axis_index("clu")
    best = []
    for local in range(CLU_DEV):
        rows = jnp.concatenate(
            [row_refs[n][start + local * most:start + (local + 1) * most] for n, start in where],
            axis=0,
        )
        best.append(best_over(rows, rows, 0))
    share = LANES // most
    group = lax.broadcasted_iota(jnp.int32, (1, LANES), 1) // most
    for base in range(0, len(where), share):
        lane = base * most
        low = best[0][:, lane:lane + LANES]
        high = pltpu.roll(best[1][:, lane:lane + LANES], most, 1)
        for parity in range(2):
            line = jnp.where(group % 2 == parity, low, high)
            for k in range(base + parity, base + share, 2):
                out_ref[me ^ k] = line


def score_all_kernel(most, rows_ref, out_ref):
    groups = out_ref.shape[0]
    units = marked_units(rows_ref[...])
    best = best_over(units, units, 0, lambda i, j: ((i // most) ^ (j // most)) % CLU_DEV == 0)
    share = LANES // (CLU_DEV * most)
    for p in range(groups):
        out_ref[p] = best[:, p // share * LANES:(p // share + 1) * LANES]


def pick_kernel(most, relative, best_ref, rank_ref, cluster_ref, out_ref):
    groups = best_ref.shape[0]
    count = rank_ref.shape[1]
    me = lax.axis_index("clu")
    cluster = cluster_ref[...]
    owner = cluster // CLU_DEV
    local = cluster % CLU_DEV
    if relative:
        lane = ((owner ^ me) + local) * most + rank_ref[...]
    else:
        lane = (me * CLU_DEV + local) * most + rank_ref[...]
    lane = lane % LANES
    best = best_ref[:, 0, :]
    row = lax.broadcasted_iota(jnp.int32, (groups, LANES), 0)
    for start in range(0, count, LANES):
        index = jnp.broadcast_to(lane[:, start:start + LANES], (groups, LANES))
        table = jnp.take_along_axis(best, index, axis=1)
        mine = row == owner[:, start:start + LANES]
        out_ref[:, start:start + LANES] = jnp.sum(
            jnp.where(mine, table, 0.0), axis=0, keepdims=True
        )


def pack(embeddings, assignment, sizes, most, labels, block_of):
    count, width = embeddings.shape
    line = jax.ShapeDtypeStruct((1, count), jnp.int32)
    rows = jax.ShapeDtypeStruct((count, width), jnp.bfloat16)
    out = tuple(jax.ShapeDtypeStruct((size, width), jnp.bfloat16) for size in sizes)
    *packed, rows, position, rank, cluster = call(
        functools.partial(pack_kernel, sizes, most, labels, block_of),
        (*out, rows, line, line, line),
        (
            pltpu.with_memory_space_constraint(embeddings, pltpu.HBM),
            pltpu.with_memory_space_constraint(assignment.reshape(1, count), pltpu.HBM),
        ),
        in_specs=[HBM, HBM],
        scratch=[pltpu.SemaphoreType.DMA((2,))],
    )
    return packed, rows, position, rank, cluster


def swap(array, k):
    groups = lax.axis_size("clu")
    return lax.ppermute(array, "clu", [(i, i ^ k) for i in range(groups)])


def message_order(groups):
    chips = groups // 2
    last = chips // 2
    far = [2 * m + 1 for m in range(chips - 1, last - 1, -1)]
    near = [2 * m + 1 for m in range(last - 1, 0, -1)]
    return [*far, near[-1], 2 * last, *near[:-1], 1]


def exchange_blocks(embeddings, assignment, most, labels):
    groups = lax.axis_size("clu")
    width = embeddings.shape[1]
    block = CLU_DEV * most
    last = groups // 2
    order = message_order(groups)
    held = [[k] if k in (last, last + 1, 1) else [k, k - 1] for k in order] + [[0]]
    flat = [k for blocks in held for k in blocks]
    sizes = [block * len(blocks) for blocks in held]

    def block_of(owner):
        k = owner ^ lax.axis_index("clu")
        spot = jnp.zeros_like(k)
        for n, value in enumerate(flat):
            spot = jnp.where(k == value, n, spot)
        return spot

    ahead = 2
    packed, rows, position, rank, cluster = pack(
        embeddings, assignment, tuple(sizes[:ahead]), most, labels, block_of
    )
    packed = [*packed, *call(
        functools.partial(pack_rest_kernel, sum(sizes[:ahead]), tuple(sizes[ahead:])),
        tuple(jax.ShapeDtypeStruct((size, width), jnp.bfloat16) for size in sizes[ahead:]),
        (rows, position),
    )]
    spots = {0: (packed[-1], 0)}
    for k, message in zip(order, packed):
        arrived = swap(message, k)
        spots[k] = arrived, 0
        if message.shape[0] > block:
            spots[k - 1] = swap(arrived[block:], 1), 0
    raw = [k for blocks in held[:ahead] for k in blocks]
    units = call(
        units_kernel,
        tuple(jax.ShapeDtypeStruct((block, width), jnp.bfloat16) for _ in raw),
        tuple(spots[k][0] for k in raw),
    )
    spots.update((k, (unit, 0)) for k, unit in zip(raw, units))
    args, where = [], []
    for k in range(groups):
        array, start = spots[k]
        where.append((len(args), start))
        args.append(array)
    best = call(
        functools.partial(score_blocks_kernel, most, tuple(where)),
        jax.ShapeDtypeStruct((groups, 1, LANES), jnp.float32), args,
    )
    return best, rank, cluster


def exchange_all(embeddings, assignment, most, labels):
    groups = lax.axis_size("clu")
    width = embeddings.shape[1]
    slots = labels * most
    (packed,), _, _, rank, cluster = pack(
        embeddings, assignment, (slots,), most, labels, lambda owner: owner
    )
    arrived = lax.all_to_all(
        packed.reshape(groups, slots // groups, width), "clu",
        split_axis=0, concat_axis=0, tiled=True,
    )
    best = call(
        functools.partial(score_all_kernel, most),
        jax.ShapeDtypeStruct((groups, 1, LANES), jnp.float32), (arrived.reshape(slots, width),),
    )
    return best, rank, cluster


def uses_blocks(groups, most):
    power = groups & (groups - 1) == 0 and groups >= 16
    return power and most % 16 == 0 and LANES % (2 * most) == 0


def shards(embeddings, assignment):
    groups = lax.axis_size("clu")
    count = embeddings.shape[0]
    most = 2 * count // (CLU_DEV * groups)
    labels = CLU_DEV * groups
    relative = uses_blocks(groups, most)
    exchange = exchange_blocks if relative else exchange_all
    best, rank, cluster = exchange(embeddings, assignment, most, labels)
    returned = lax.all_to_all(best, "clu", split_axis=0, concat_axis=0, tiled=True)
    out = call(
        functools.partial(pick_kernel, most, relative),
        jax.ShapeDtypeStruct((1, count), jnp.float32), (returned, rank, cluster),
    )
    return out.reshape(count)


def solution(mesh):
    in_specs = (P(("lang", "clu"), None), P(("lang", "clu"), None))
    out_specs = P(("lang", "clu"))

    return jax.shard_map(shards, mesh=mesh, in_specs=in_specs, out_specs=out_specs, check_vma=False)
```

```python
import functools

import jax
import jax.numpy as jnp
from jax import lax
from jax.experimental import pallas as pl
from jax.experimental.pallas import tpu as pltpu
from jax.sharding import PartitionSpec as P


CLU_DEV = 2
EPS = 1e-06
PAD = 2.0
RAW_PAD = 64.0
LANES = 128
GRANT = 12 * 1024 * 1024
VMEM = pl.BlockSpec(memory_space=pltpu.VMEM)
HBM = pl.BlockSpec(memory_space=pltpu.HBM)


def call(kernel, out_shape, args, in_specs=None, scratch=(), flops=1 << 24, grant=GRANT):
    return pl.pallas_call(
        kernel,
        out_shape=out_shape,
        in_specs=in_specs or [VMEM] * len(args),
        out_specs=jax.tree.map(lambda _: VMEM, out_shape),
        scratch_shapes=scratch,
        compiler_params=pltpu.CompilerParams(vmem_limit_bytes=grant),
        cost_estimate=pl.CostEstimate(flops=flops, bytes_accessed=1 << 20, transcendentals=0),
    )(*args)


def rank_of(cluster, labels):
    count = cluster.shape[1]
    member = lax.broadcasted_iota(jnp.int32, (labels, count), 0) == cluster
    before = (
        lax.broadcasted_iota(jnp.int32, (count, count), 0)
        < lax.broadcasted_iota(jnp.int32, (count, count), 1)
    ).astype(jnp.bfloat16)
    prior = jnp.dot(member.astype(jnp.bfloat16), before, preferred_element_type=jnp.float32)
    return jnp.sum(jnp.where(member, prior, 0.0), axis=0, keepdims=True).astype(jnp.int32)


def unit_rows(rows):
    values = rows.astype(jnp.float32)
    scale = lax.rsqrt(jnp.sum(values * values, axis=-1, keepdims=True) + EPS)
    return (values * scale).astype(jnp.bfloat16)


def place_rows(first, sizes, position, rows, pad, out_refs):
    slots = sum(sizes)
    count = rows.shape[0]
    place = lax.broadcasted_iota(jnp.int32, (slots, count), 0) + first == position
    live = jnp.sum(place.astype(jnp.float32), axis=1, keepdims=True) > 0
    packed = jnp.dot(place.astype(jnp.bfloat16), rows, preferred_element_type=jnp.float32)
    column = lax.broadcasted_iota(jnp.int32, (slots, LANES), 1) == 0
    head = jnp.where(column & ~live, pad, packed[:, :LANES]).astype(jnp.bfloat16)
    rest = packed[:, LANES:].astype(jnp.bfloat16)
    start = 0
    for size, out_ref in zip(sizes, out_refs):
        out_ref[:, :LANES] = head[start:start + size]
        out_ref[:, LANES:] = rest[start:start + size]
        start += size


def pack_kernel(sizes, most, labels, block_of, rows_hbm, cluster_hbm, *refs):
    *out_refs, rows_ref, position_ref, rank_ref, cluster_ref, sems = refs
    load_cluster = pltpu.make_async_copy(cluster_hbm, cluster_ref, sems.at[0])
    load_rows = pltpu.make_async_copy(rows_hbm, rows_ref, sems.at[1])
    load_cluster.start()
    load_rows.start()
    load_cluster.wait()
    cluster = cluster_ref[...]
    rank = rank_of(cluster, labels)
    rank_ref[...] = rank
    owner = block_of(cluster // CLU_DEV)
    position = (owner * CLU_DEV + cluster % CLU_DEV) * most + rank
    position_ref[...] = position
    load_rows.wait()
    place_rows(0, sizes, position, rows_ref[...], RAW_PAD, out_refs)


def pack_rest_kernel(first, sizes, rows_ref, position_ref, *out_refs):
    place_rows(first, sizes, position_ref[...], unit_rows(rows_ref[...]), PAD, out_refs)


def fits(rows, limit):
    return rows[:, :1].astype(jnp.float32) < limit


def marked_units(rows):
    live = fits(rows, RAW_PAD / 2)
    unit = unit_rows(rows)
    column = lax.broadcasted_iota(jnp.int32, (rows.shape[0], LANES), 1) == 0
    head = jnp.where(column & ~live, PAD, unit[:, :LANES].astype(jnp.float32))
    return jnp.concatenate([head.astype(jnp.bfloat16), unit[:, LANES:]], axis=1)


def best_over(left, right, offset, keep=None):
    gram = lax.dot_general(
        left, right, (((1,), (1,)), ((), ())), preferred_element_type=jnp.float32
    )
    i = lax.broadcasted_iota(jnp.int32, gram.shape, 0)
    j = lax.broadcasted_iota(jnp.int32, gram.shape, 1)
    mask = fits(left, PAD * 0.75) & (i + offset != j)
    if keep is not None:
        mask &= keep(i, j)
    return jnp.max(jnp.where(mask, gram, -1.0), axis=0, keepdims=True)


def units_kernel(*refs):
    half = len(refs) // 2
    for row_ref, out_ref in zip(refs[:half], refs[half:]):
        out_ref[...] = marked_units(row_ref[:out_ref.shape[0]])


def score_blocks_kernel(most, where, *refs):
    *row_refs, out_ref = refs
    me = lax.axis_index("clu")
    best = []
    for local in range(CLU_DEV):
        rows = jnp.concatenate(
            [row_refs[n][start + local * most:start + (local + 1) * most] for n, start in where],
            axis=0,
        )
        best.append(best_over(rows, rows, 0))
    share = LANES // most
    group = lax.broadcasted_iota(jnp.int32, (1, LANES), 1) // most
    for base in range(0, len(where), share):
        lane = base * most
        low = best[0][:, lane:lane + LANES]
        high = pltpu.roll(best[1][:, lane:lane + LANES], most, 1)
        for parity in range(2):
            line = jnp.where(group % 2 == parity, low, high)
            for k in range(base + parity, base + share, 2):
                out_ref[me ^ k] = line


def score_all_kernel(most, rows_ref, out_ref):
    groups = out_ref.shape[0]
    units = marked_units(rows_ref[...])
    best = best_over(units, units, 0, lambda i, j: ((i // most) ^ (j // most)) % CLU_DEV == 0)
    share = LANES // (CLU_DEV * most)
    for p in range(groups):
        out_ref[p] = best[:, p // share * LANES:(p // share + 1) * LANES]


def pick_kernel(most, relative, best_ref, rank_ref, cluster_ref, out_ref):
    groups = best_ref.shape[0]
    count = rank_ref.shape[1]
    me = lax.axis_index("clu")
    cluster = cluster_ref[...]
    owner = cluster // CLU_DEV
    local = cluster % CLU_DEV
    if relative:
        lane = ((owner ^ me) + local) * most + rank_ref[...]
    else:
        lane = (me * CLU_DEV + local) * most + rank_ref[...]
    lane = lane % LANES
    best = best_ref[:, 0, :]
    row = lax.broadcasted_iota(jnp.int32, (groups, LANES), 0)
    for start in range(0, count, LANES):
        index = jnp.broadcast_to(lane[:, start:start + LANES], (groups, LANES))
        table = jnp.take_along_axis(best, index, axis=1)
        mine = row == owner[:, start:start + LANES]
        out_ref[:, start:start + LANES] = jnp.sum(
            jnp.where(mine, table, 0.0), axis=0, keepdims=True
        )


def pack(embeddings, assignment, sizes, most, labels, block_of):
    count, width = embeddings.shape
    line = jax.ShapeDtypeStruct((1, count), jnp.int32)
    rows = jax.ShapeDtypeStruct((count, width), jnp.bfloat16)
    out = tuple(jax.ShapeDtypeStruct((size, width), jnp.bfloat16) for size in sizes)
    *packed, rows, position, rank, cluster = call(
        functools.partial(pack_kernel, sizes, most, labels, block_of),
        (*out, rows, line, line, line),
        (
            pltpu.with_memory_space_constraint(embeddings, pltpu.HBM),
            pltpu.with_memory_space_constraint(assignment.reshape(1, count), pltpu.HBM),
        ),
        in_specs=[HBM, HBM],
        scratch=[pltpu.SemaphoreType.DMA((2,))],
    )
    return packed, rows, position, rank, cluster


def swap(array, k):
    groups = lax.axis_size("clu")
    return lax.ppermute(array, "clu", [(i, i ^ k) for i in range(groups)])


def message_order(groups):
    chips = groups // 2
    last = groups - 2
    far = [2 * m + 1 for m in range(chips - 2, chips // 2 - 1, -1)]
    near = [2 * m + 1 for m in range(2, chips // 2)]
    return [*far, *near, last + 1, 3, last, 1]


def exchange_blocks(embeddings, assignment, most, labels):
    groups = lax.axis_size("clu")
    width = embeddings.shape[1]
    block = CLU_DEV * most
    last = groups - 2
    order = message_order(groups)
    held = [[k] if k in (last, last + 1, 1) else [k, k - 1] for k in order] + [[0]]
    flat = [k for blocks in held for k in blocks]
    sizes = [block * len(blocks) for blocks in held]

    def block_of(owner):
        k = owner ^ lax.axis_index("clu")
        spot = jnp.zeros_like(k)
        for n, value in enumerate(flat):
            spot = jnp.where(k == value, n, spot)
        return spot

    ahead = 1
    packed, rows, position, rank, cluster = pack(
        embeddings, assignment, tuple(sizes[:ahead]), most, labels, block_of
    )
    packed = [*packed, *call(
        functools.partial(pack_rest_kernel, sum(sizes[:ahead]), tuple(sizes[ahead:])),
        tuple(jax.ShapeDtypeStruct((size, width), jnp.bfloat16) for size in sizes[ahead:]),
        (rows, position),
    )]
    spots = {0: (packed[-1], 0)}
    for k, message in zip(order, packed):
        arrived = swap(message, k)
        spots[k] = arrived, 0
        if message.shape[0] > block:
            spots[k - 1] = swap(arrived[block:], 1), 0
    raw = [k for blocks in held[:ahead] for k in blocks]
    units = call(
        units_kernel,
        tuple(jax.ShapeDtypeStruct((block, width), jnp.bfloat16) for _ in raw),
        tuple(spots[k][0] for k in raw),
    )
    spots.update((k, (unit, 0)) for k, unit in zip(raw, units))
    args, where = [], []
    for k in range(groups):
        array, start = spots[k]
        where.append((len(args), start))
        args.append(array)
    best = call(
        functools.partial(score_blocks_kernel, most, tuple(where)),
        jax.ShapeDtypeStruct((groups, 1, LANES), jnp.float32), args,
    )
    return best, rank, cluster


def exchange_all(embeddings, assignment, most, labels):
    groups = lax.axis_size("clu")
    width = embeddings.shape[1]
    slots = labels * most
    (packed,), _, _, rank, cluster = pack(
        embeddings, assignment, (slots,), most, labels, lambda owner: owner
    )
    arrived = lax.all_to_all(
        packed.reshape(groups, slots // groups, width), "clu",
        split_axis=0, concat_axis=0, tiled=True,
    )
    best = call(
        functools.partial(score_all_kernel, most),
        jax.ShapeDtypeStruct((groups, 1, LANES), jnp.float32), (arrived.reshape(slots, width),),
    )
    return best, rank, cluster


def uses_blocks(groups, most):
    power = groups & (groups - 1) == 0 and groups >= 16
    return power and most % 16 == 0 and LANES % (2 * most) == 0


def shards(embeddings, assignment):
    groups = lax.axis_size("clu")
    count = embeddings.shape[0]
    most = 2 * count // (CLU_DEV * groups)
    labels = CLU_DEV * groups
    relative = uses_blocks(groups, most)
    exchange = exchange_blocks if relative else exchange_all
    best, rank, cluster = exchange(embeddings, assignment, most, labels)
    returned = lax.all_to_all(best, "clu", split_axis=0, concat_axis=0, tiled=True)
    out = call(
        functools.partial(pick_kernel, most, relative),
        jax.ShapeDtypeStruct((1, count), jnp.float32), (returned, rank, cluster),
    )
    return out.reshape(count)


def solution(mesh):
    in_specs = (P(("lang", "clu"), None), P(("lang", "clu"), None))
    out_specs = P(("lang", "clu"))

    return jax.shard_map(shards, mesh=mesh, in_specs=in_specs, out_specs=out_specs, check_vma=False)
```

```python
import functools

import jax
import jax.numpy as jnp
from jax import lax
from jax.experimental import pallas as pl
from jax.experimental.pallas import tpu as pltpu
from jax.sharding import PartitionSpec as P


CLU_DEV = 2
EPS = 1e-06
PAD = 2.0
RAW_PAD = 64.0
LANES = 128
GRANT = 12 * 1024 * 1024
VMEM = pl.BlockSpec(memory_space=pltpu.VMEM)
HBM = pl.BlockSpec(memory_space=pltpu.HBM)


def call(kernel, out_shape, args, in_specs=None, scratch=(), flops=1 << 24, grant=GRANT):
    return pl.pallas_call(
        kernel,
        out_shape=out_shape,
        in_specs=in_specs or [VMEM] * len(args),
        out_specs=jax.tree.map(lambda _: VMEM, out_shape),
        scratch_shapes=scratch,
        compiler_params=pltpu.CompilerParams(vmem_limit_bytes=grant),
        cost_estimate=pl.CostEstimate(flops=flops, bytes_accessed=1 << 20, transcendentals=0),
    )(*args)


def rank_of(cluster, labels):
    count = cluster.shape[1]
    member = lax.broadcasted_iota(jnp.int32, (labels, count), 0) == cluster
    before = (
        lax.broadcasted_iota(jnp.int32, (count, count), 0)
        < lax.broadcasted_iota(jnp.int32, (count, count), 1)
    ).astype(jnp.bfloat16)
    prior = jnp.dot(member.astype(jnp.bfloat16), before, preferred_element_type=jnp.float32)
    return jnp.sum(jnp.where(member, prior, 0.0), axis=0, keepdims=True).astype(jnp.int32)


def unit_rows(rows):
    values = rows.astype(jnp.float32)
    scale = lax.rsqrt(jnp.sum(values * values, axis=-1, keepdims=True) + EPS)
    return (values * scale).astype(jnp.bfloat16)


def place_rows(first, sizes, position, rows, pad, out_refs):
    slots = sum(sizes)
    count = rows.shape[0]
    place = lax.broadcasted_iota(jnp.int32, (slots, count), 0) + first == position
    live = jnp.sum(place.astype(jnp.float32), axis=1, keepdims=True) > 0
    packed = jnp.dot(place.astype(jnp.bfloat16), rows, preferred_element_type=jnp.float32)
    column = lax.broadcasted_iota(jnp.int32, (slots, LANES), 1) == 0
    head = jnp.where(column & ~live, pad, packed[:, :LANES]).astype(jnp.bfloat16)
    rest = packed[:, LANES:].astype(jnp.bfloat16)
    start = 0
    for size, out_ref in zip(sizes, out_refs):
        out_ref[:, :LANES] = head[start:start + size]
        out_ref[:, LANES:] = rest[start:start + size]
        start += size


def pack_kernel(sizes, most, labels, block_of, rows_hbm, cluster_hbm, *refs):
    *out_refs, rows_ref, position_ref, rank_ref, cluster_ref, sems = refs
    load_cluster = pltpu.make_async_copy(cluster_hbm, cluster_ref, sems.at[0])
    load_rows = pltpu.make_async_copy(rows_hbm, rows_ref, sems.at[1])
    load_cluster.start()
    load_rows.start()
    load_cluster.wait()
    cluster = cluster_ref[...]
    rank = rank_of(cluster, labels)
    rank_ref[...] = rank
    owner = block_of(cluster // CLU_DEV)
    position = (owner * CLU_DEV + cluster % CLU_DEV) * most + rank
    position_ref[...] = position
    load_rows.wait()
    place_rows(0, sizes, position, rows_ref[...], RAW_PAD, out_refs)


def pack_rest_kernel(first, sizes, rows_ref, position_ref, *out_refs):
    place_rows(first, sizes, position_ref[...], unit_rows(rows_ref[...]), PAD, out_refs)


def fits(rows, limit):
    return rows[:, :1].astype(jnp.float32) < limit


def marked_units(rows):
    live = fits(rows, RAW_PAD / 2)
    unit = unit_rows(rows)
    column = lax.broadcasted_iota(jnp.int32, (rows.shape[0], LANES), 1) == 0
    head = jnp.where(column & ~live, PAD, unit[:, :LANES].astype(jnp.float32))
    return jnp.concatenate([head.astype(jnp.bfloat16), unit[:, LANES:]], axis=1)


def best_over(left, right, offset, keep=None):
    gram = lax.dot_general(
        left, right, (((1,), (1,)), ((), ())), preferred_element_type=jnp.float32
    )
    i = lax.broadcasted_iota(jnp.int32, gram.shape, 0)
    j = lax.broadcasted_iota(jnp.int32, gram.shape, 1)
    mask = fits(left, PAD * 0.75) & (i + offset != j)
    if keep is not None:
        mask &= keep(i, j)
    return jnp.max(jnp.where(mask, gram, -1.0), axis=0, keepdims=True)


def units_kernel(*refs):
    half = len(refs) // 2
    for row_ref, out_ref in zip(refs[:half], refs[half:]):
        out_ref[...] = marked_units(row_ref[:out_ref.shape[0]])


def score_blocks_kernel(most, where, *refs):
    *row_refs, out_ref = refs
    me = lax.axis_index("clu")
    best = []
    for local in range(CLU_DEV):
        rows = jnp.concatenate(
            [row_refs[n][start + local * most:start + (local + 1) * most] for n, start in where],
            axis=0,
        )
        best.append(best_over(rows, rows, 0))
    share = LANES // most
    group = lax.broadcasted_iota(jnp.int32, (1, LANES), 1) // most
    for base in range(0, len(where), share):
        lane = base * most
        low = best[0][:, lane:lane + LANES]
        high = pltpu.roll(best[1][:, lane:lane + LANES], most, 1)
        for parity in range(2):
            line = jnp.where(group % 2 == parity, low, high)
            for k in range(base + parity, base + share, 2):
                out_ref[me ^ k] = line


def score_all_kernel(most, rows_ref, out_ref):
    groups = out_ref.shape[0]
    units = marked_units(rows_ref[...])
    best = best_over(units, units, 0, lambda i, j: ((i // most) ^ (j // most)) % CLU_DEV == 0)
    share = LANES // (CLU_DEV * most)
    for p in range(groups):
        out_ref[p] = best[:, p // share * LANES:(p // share + 1) * LANES]


def pick_kernel(most, relative, best_ref, rank_ref, cluster_ref, out_ref):
    groups = best_ref.shape[0]
    count = rank_ref.shape[1]
    me = lax.axis_index("clu")
    cluster = cluster_ref[...]
    owner = cluster // CLU_DEV
    local = cluster % CLU_DEV
    if relative:
        lane = ((owner ^ me) + local) * most + rank_ref[...]
    else:
        lane = (me * CLU_DEV + local) * most + rank_ref[...]
    lane = lane % LANES
    best = best_ref[:, 0, :]
    row = lax.broadcasted_iota(jnp.int32, (groups, LANES), 0)
    for start in range(0, count, LANES):
        index = jnp.broadcast_to(lane[:, start:start + LANES], (groups, LANES))
        table = jnp.take_along_axis(best, index, axis=1)
        mine = row == owner[:, start:start + LANES]
        out_ref[:, start:start + LANES] = jnp.sum(
            jnp.where(mine, table, 0.0), axis=0, keepdims=True
        )


def pack(embeddings, assignment, sizes, most, labels, block_of):
    count, width = embeddings.shape
    line = jax.ShapeDtypeStruct((1, count), jnp.int32)
    rows = jax.ShapeDtypeStruct((count, width), jnp.bfloat16)
    out = tuple(jax.ShapeDtypeStruct((size, width), jnp.bfloat16) for size in sizes)
    *packed, rows, position, rank, cluster = call(
        functools.partial(pack_kernel, sizes, most, labels, block_of),
        (*out, rows, line, line, line),
        (
            pltpu.with_memory_space_constraint(embeddings, pltpu.HBM),
            pltpu.with_memory_space_constraint(assignment.reshape(1, count), pltpu.HBM),
        ),
        in_specs=[HBM, HBM],
        scratch=[pltpu.SemaphoreType.DMA((2,))],
    )
    return packed, rows, position, rank, cluster


def swap(array, k):
    groups = lax.axis_size("clu")
    return lax.ppermute(array, "clu", [(i, i ^ k) for i in range(groups)])


def message_order(groups):
    chips = groups // 2
    last = groups - 4
    far = [2 * m + 1 for m in (chips - 1, *range(chips - 3, chips // 2 - 1, -1))]
    near = [2 * m + 1 for m in range(chips // 2 - 1, 0, -1)]
    return [*far, *near, last + 1, last, 1]


def exchange_blocks(embeddings, assignment, most, labels):
    groups = lax.axis_size("clu")
    width = embeddings.shape[1]
    block = CLU_DEV * most
    last = groups - 4
    order = message_order(groups)
    held = [[k] if k in (last, last + 1, 1) else [k, k - 1] for k in order] + [[0]]
    flat = [k for blocks in held for k in blocks]
    sizes = [block * len(blocks) for blocks in held]

    def block_of(owner):
        k = owner ^ lax.axis_index("clu")
        spot = jnp.zeros_like(k)
        for n, value in enumerate(flat):
            spot = jnp.where(k == value, n, spot)
        return spot

    ahead = 1
    packed, rows, position, rank, cluster = pack(
        embeddings, assignment, tuple(sizes[:ahead]), most, labels, block_of
    )
    packed = [*packed, *call(
        functools.partial(pack_rest_kernel, sum(sizes[:ahead]), tuple(sizes[ahead:])),
        tuple(jax.ShapeDtypeStruct((size, width), jnp.bfloat16) for size in sizes[ahead:]),
        (rows, position),
    )]
    spots = {0: (packed[-1], 0)}
    for k, message in zip(order, packed):
        arrived = swap(message, k)
        spots[k] = arrived, 0
        if message.shape[0] > block:
            spots[k - 1] = swap(arrived[block:], 1), 0
    raw = [k for blocks in held[:ahead] for k in blocks]
    units = call(
        units_kernel,
        tuple(jax.ShapeDtypeStruct((block, width), jnp.bfloat16) for _ in raw),
        tuple(spots[k][0] for k in raw),
    )
    spots.update((k, (unit, 0)) for k, unit in zip(raw, units))
    args, where = [], []
    for k in range(groups):
        array, start = spots[k]
        where.append((len(args), start))
        args.append(array)
    best = call(
        functools.partial(score_blocks_kernel, most, tuple(where)),
        jax.ShapeDtypeStruct((groups, 1, LANES), jnp.float32), args,
    )
    return best, rank, cluster


def exchange_all(embeddings, assignment, most, labels):
    groups = lax.axis_size("clu")
    width = embeddings.shape[1]
    slots = labels * most
    (packed,), _, _, rank, cluster = pack(
        embeddings, assignment, (slots,), most, labels, lambda owner: owner
    )
    arrived = lax.all_to_all(
        packed.reshape(groups, slots // groups, width), "clu",
        split_axis=0, concat_axis=0, tiled=True,
    )
    best = call(
        functools.partial(score_all_kernel, most),
        jax.ShapeDtypeStruct((groups, 1, LANES), jnp.float32), (arrived.reshape(slots, width),),
    )
    return best, rank, cluster


def uses_blocks(groups, most):
    power = groups & (groups - 1) == 0 and groups >= 16
    return power and most % 16 == 0 and LANES % (2 * most) == 0


def shards(embeddings, assignment):
    groups = lax.axis_size("clu")
    count = embeddings.shape[0]
    most = 2 * count // (CLU_DEV * groups)
    labels = CLU_DEV * groups
    relative = uses_blocks(groups, most)
    exchange = exchange_blocks if relative else exchange_all
    best, rank, cluster = exchange(embeddings, assignment, most, labels)
    returned = lax.all_to_all(best, "clu", split_axis=0, concat_axis=0, tiled=True)
    out = call(
        functools.partial(pick_kernel, most, relative),
        jax.ShapeDtypeStruct((1, count), jnp.float32), (returned, rank, cluster),
    )
    return out.reshape(count)


def solution(mesh):
    in_specs = (P(("lang", "clu"), None), P(("lang", "clu"), None))
    out_specs = P(("lang", "clu"))

    return jax.shard_map(shards, mesh=mesh, in_specs=in_specs, out_specs=out_specs, check_vma=False)
```
